512 devices in a mesh: dp: 32 (over z_lo, x), tensor: 16 (over z_hi, y, core).
Axes of the slice: x: 4, y: 4, z: 16 (z_hi: 2, z_lo: 8; z = z_hi * 8 + z_lo), core: 2. Of those that a mesh axis runs over, the one named last changes fastest.
Arguments:
- hidden: bfloat16 [8192, 14336], P('dp', 'tensor'), parts along dimension 0, may hold values from -16 to 16
- signs: int32 [14336], P('tensor'), may hold values 0 or 1
- packed: int32 [14336, 512], P('tensor'), may hold values from -2147483648 to 2147483646
- group_scales: int32 [112, 4096], P('tensor'), may hold values from 1 to 16
- residual: bfloat16 [8192, 4096], P(('dp', 'tensor')), parts along dimension 0, may hold values from -16 to 16
Outputs:
- new_residual: bfloat16 [8192, 4096], P(('dp', 'tensor')), parts along dimension 0
- normed: bfloat16 [8192, 4096], P(('dp', 'tensor')), parts along dimension 0
The draws below stay inside these ranges and needn't reach their ends.
There are 32 independent parts, one for each index of `dp`. The reference program is written for one: setup_inputs(seed, part) draws one part's arguments, and reference() takes and returns one part's arrays. A program takes and returns all parts, laid end to end along the dimension named above; an argument that names none is the same for every part. Nothing has to cross between parts.
Inputs may be any that keep to these rules, and one draw needn't show every extreme that they name: `packed`: bits 4 k to 4 k + 3 of word j in row f hold the code of output feature k * 512 + j plus 8.
All inputs are finite; a program needn't handle non-finite values. No bound on the sum of `signs` on one device may be relied on, other than what follows from the above.
Results may differ from the reference program's by a relative error of at most 0.0054.
Values may be sent and summed in bfloat16 or wider, within the bound.
A program may use at most 64 MiB of HBM per device.

```python
import math
import jax
import jax.numpy as jnp
import numpy as np
from jax import lax

D = 4096
FF = 14336
GROUP = 128
ROWS = 256


def scaled_draw(key, count, width):
    first = jax.random.fold_in(key, 0)
    third = jax.random.fold_in(key, 2)
    column_scale = jnp.exp(jax.random.uniform(first, (1, width), jnp.float32, math.log(0.3), math.log(3.0)))
    values = jax.random.normal(third, (count, width), jnp.float32) * column_scale
    return jnp.clip(values, -16.0, 16.0)


def draw_hidden(key, part):
    return scaled_draw(jax.random.fold_in(key, 11), ROWS, FF).astype(jnp.bfloat16)


def draw_residual(key, part):
    return scaled_draw(jax.random.fold_in(key, 23), ROWS, D).astype(jnp.bfloat16)


def touch_ends(values, rng, low, high):
    spot = [jax.random.randint(jax.random.fold_in(rng, axis), (), 0, length) for axis, length in enumerate(values.shape)]
    main_axis = values.shape.index(max(values.shape))
    beside = spot[:main_axis] + [(spot[main_axis] + 1) % values.shape[main_axis]] + spot[main_axis + 1:]
    return values.at[tuple(spot)].set(low).at[tuple(beside)].set(high)


def setup_inputs(seed: int = 0, part: int = 0) -> dict:
    key_of = jax.random.split(jax.random.key(seed), 6)
    own_keys = jax.random.split(jax.random.fold_in(key_of[5], part), 6)
    hidden = draw_hidden(jax.random.fold_in(jax.random.fold_in(key_of[5], part), 71), part)
    signs = touch_ends((jax.random.randint(key_of[1], (FF,), 0, 2) < 1).astype(jnp.int32), jax.random.fold_in(key_of[1], 1), 0, 1)
    packed = touch_ends(jax.random.randint(key_of[2], (FF, D // 8), -2147483648, 2147483647), jax.random.fold_in(key_of[2], 1), -2147483648, 2147483646).astype(jnp.int32)
    group_scales = touch_ends(jax.random.randint(key_of[3], (FF // GROUP, D), 1, 17), jax.random.fold_in(key_of[3], 1), 1, 16).astype(jnp.int32)
    residual = draw_residual(jax.random.fold_in(jax.random.fold_in(key_of[5], part), 71), part)
    return {"hidden": hidden, "signs": signs, "packed": packed, "group_scales": group_scales, "residual": residual}


def paley_table():
    offsets = (np.arange(13)[None, :] - np.arange(13)[:, None]) % 13
    residues = np.zeros(13)
    residues[np.arange(1, 13) ** 2 % 13] = 1.0
    quadratic = np.where(offsets == 0, 0.0, np.where(residues[offsets] > 0, 1.0, -1.0))
    conference = np.zeros((14, 14))
    conference[0, 1:] = 1.0
    conference[1:, 0] = 1.0
    conference[1:, 1:] = quadratic
    upper = np.array([[1.0, 1.0], [1.0, -1.0]])
    lower = np.array([[1.0, -1.0], [-1.0, -1.0]])
    return np.kron(conference, upper) + np.kron(np.eye(14), lower)

def sylvester(order):
    first = lax.broadcasted_iota(jnp.int32, (order, order), 0)
    second = lax.broadcasted_iota(jnp.int32, (order, order), 1)
    common = first & second
    parity = jnp.zeros((order, order), jnp.int32)
    for bit in range(max(order.bit_length() - 1, 0)):
        parity = parity ^ jnp.right_shift(common, bit) & 1
    return (1 - 2 * parity).astype(jnp.float32)

def reference(hidden, signs, packed, group_scales, residual):
    count = hidden.shape[0]
    flips = (2 * signs - 1).astype(jnp.float32)
    signed = hidden.astype(jnp.float32) * flips[None, :]
    blocks = signed.reshape(count, FF // 28, 28)
    outer = sylvester(FF // 28)
    inner = jnp.asarray(paley_table(), jnp.float32)
    mixed = jnp.einsum('rba,cb->rca', blocks, outer, precision=lax.Precision.HIGHEST)
    mixed = jnp.einsum('rca,da->rcd', mixed, inner, precision=lax.Precision.HIGHEST)
    rotated = (mixed.reshape(count, FF) * (1.0 / math.sqrt(FF))).astype(jnp.bfloat16)
    width = D // 8
    pieces = []
    for nibble in range(8):
        codes = (jnp.right_shift(packed, 4 * nibble) & 15) - 8
        scales = group_scales[:, nibble * width:(nibble + 1) * width]
        weights = (codes.reshape(FF // GROUP, GROUP, width) * scales[:, None, :]).reshape(FF, width)
        pieces.append(jnp.dot(rotated, weights.astype(jnp.bfloat16), preferred_element_type=jnp.float32))
    branch = jnp.concatenate(pieces, axis=1) * (1.0 / (45.0 * math.sqrt(FF)))
    new_residual = (residual.astype(jnp.float32) + branch).astype(jnp.bfloat16)
    values = new_residual.astype(jnp.float32)
    normed = values * lax.rsqrt(lax.optimization_barrier(jnp.mean(values * values, axis=1, keepdims=True)) + 1e-05)
    return (new_residual, normed.astype(jnp.bfloat16))
```

```python
import functools
import math

import jax
import jax.numpy as jnp
import numpy as np
from jax import lax
from jax.experimental import pallas as pl
from jax.experimental.pallas import tpu as pltpu
from jax.sharding import PartitionSpec as P

FF = 14336
D = 4096
LOCAL = 896
WORDS = 512
GROUPS = 7
CHUNKS = 4
BLOCKS = 4
COLS = D // BLOCKS
MESH = pl.DeviceIdType.MESH
UNIT = 1.0 / math.sqrt(FF)
BRANCH = 1.0 / (45.0 * math.sqrt(FF))
F32 = jnp.float32
BF16 = jnp.bfloat16


def paley_table():
    offsets = (np.arange(13)[None, :] - np.arange(13)[:, None]) % 13
    residues = np.zeros(13)
    residues[np.arange(1, 13) ** 2 % 13] = 1.0
    quadratic = np.where(offsets == 0, 0.0, np.where(residues[offsets] > 0, 1.0, -1.0))
    conference = np.zeros((14, 14))
    conference[0, 1:] = 1.0
    conference[1:, 0] = 1.0
    conference[1:, 1:] = quadratic
    upper = np.array([[1.0, 1.0], [1.0, -1.0]])
    lower = np.array([[1.0, -1.0], [-1.0, -1.0]])
    return np.kron(conference, upper) + np.kron(np.eye(14), lower)


def sylvester(order):
    table = np.ones((1, 1))
    while table.shape[0] < order:
        table = np.kron(np.array([[1.0, 1.0], [1.0, -1.0]]), table)
    return table


def sign_of(bits):
    odd = lax.rem(bits + bits // 2, 2)
    return 1.0 - 2.0 * odd.astype(F32)


def kernel(
    hidden,
    signs,
    packed,
    scales,
    residual,
    table_hbm,
    new_out,
    norm_out,
    h,
    zin,
    sg,
    pk,
    sc,
    res,
    table,
    wts,
    v,
    vr,
    w,
    wr,
    p,
    pr,
    q,
    qr,
    r1,
    r1r,
    acc,
    local_sem,
    zin_s,
    zin_r,
    sg_s,
    sg_r,
    v_s,
    v_r,
    w_s,
    w_r,
    p_s,
    p_r,
    q_s,
    q_r,
    o_s,
    o_r,
):
    dp = lax.axis_index("dp")
    t = lax.axis_index("tensor")
    z = t // 8
    y = lax.rem(t // 2, 4)
    c = lax.rem(t, 2)

    def dev(zz, yy, cc):
        return (dp, zz * 8 + yy * 2 + cc)

    far = dev(1 - z, y, c)
    twin = dev(z, y, 1 - c)
    ring = [dev(z, lax.rem(y + d, 4), c) for d in (1, 2, 3)]

    loads = [
        pltpu.make_async_copy(hidden, h, local_sem.at[0]),
        pltpu.make_async_copy(signs, sg.at[0], local_sem.at[1]),
        pltpu.make_async_copy(packed, pk, local_sem.at[2]),
        pltpu.make_async_copy(scales, sc, local_sem.at[3]),
        pltpu.make_async_copy(table_hbm, table, local_sem.at[4]),
        pltpu.make_async_copy(residual, res, local_sem.at[5]),
    ]
    for load in loads:
        load.start()

    barrier = pltpu.get_barrier_semaphore()
    for peer in [far, twin] + ring:
        pl.semaphore_signal(barrier, 1, device_id=peer, device_id_type=MESH)
    pl.semaphore_wait(barrier, 5)

    def remote(src, dst, ss, rs, peer):
        return pltpu.make_async_remote_copy(
            src_ref=src, dst_ref=dst, send_sem=ss, recv_sem=rs, device_id=peer, device_id_type=MESH
        )

    loads[1].wait()
    sg_copy = remote(sg.at[0], sg.at[1], sg_s, sg_r, far)
    sg_copy.start()
    loads[0].wait()
    zin_copies = []
    for k in range(CHUNKS):
        half = z if k < 2 else 1 - z
        copy = remote(h.at[half, :, :, k % 2], zin.at[k], zin_s.at[k], zin_r.at[k], far)
        copy.start()
        zin_copies.append(copy)

    loads[2].wait()
    loads[3].wait()

    def dequantize(i, carry):
        rows = pl.ds(pl.multiple_of(i * 16, 16), 16)
        words = pk[rows, :] ^ jnp.int32(-2004318072)
        for k in range(8):
            codes = jnp.right_shift(jnp.left_shift(words, 28 - 4 * k), 28)
            scale = sc[pl.ds(i // 8, 1), k * WORDS : (k + 1) * WORDS]
            value = (codes.astype(F32) * scale.astype(F32)).astype(BF16)
            wts[k // 2, rows, (k % 2) * WORDS : (k % 2 + 1) * WORDS] = value
        return carry

    lax.fori_loop(0, LOCAL // 16, dequantize, 0)
    loads[4].wait()

    sg_copy.wait()
    flips = (2 * sg[...] - 1).astype(F32)
    own_flip = flips[0] * (1 - 2 * z).astype(F32)
    far_flip = flips[1]

    v_copies, w_copies, p_copies, q_copies, o_copies = {}, {}, {}, {}, {}

    def combine_far(k):
        half = 1 - z if k < 2 else z
        zin_copies[k].wait_recv()
        for g in range(GROUPS):
            lanes = slice(g * 128, (g + 1) * 128)
            own = h[half, :, :, k % 2, :, lanes].astype(F32)
            other = zin[k, :, :, :, lanes].astype(F32)
            v[k, :, :, :, lanes] = own * own_flip[g : g + 1] + other * far_flip[g : g + 1]
        v_copies[k] = remote(v.at[k], vr.at[k], v_s.at[k], v_r.at[k], twin)
        v_copies[k].start()

    def combine_twin(k):
        v_copies[k].wait_recv()
        w[k] = (vr[k] + v[k] * (1 - 2 * c).astype(F32)).astype(BF16)
        for d in range(3):
            w_copies[k, d] = remote(w.at[k], wr.at[k, d], w_s.at[k, d], w_r.at[k, d], ring[d])
            w_copies[k, d].start()

    def p_copy(k, j):
        return remote(p.at[k, j, :, 1 - c], pr.at[k, j], p_s.at[k, j], p_r.at[k, j], twin)

    def q_copy(k, j, d):
        return remote(
            q.at[k, j, lax.rem(y + d + 1, 4)], qr.at[k, j, d], q_s.at[k, j, d], q_r.at[k, j, d], ring[d]
        )

    def multiply(k):
        for d in range(3):
            w_copies[k, d].wait_recv()
        u = w[k].astype(F32) * sign_of(y)
        for d in range(3):
            source = lax.rem(y + 3 - d, 4)
            u = u + wr[k, d].astype(F32) * sign_of(y & source)
        u = u.reshape(64, LOCAL).astype(BF16)
        rotated = (jnp.dot(u, table[...], preferred_element_type=F32) * UNIT).astype(BF16)

        def block(j, carry):
            @pl.when(j < BLOCKS)
            def _():
                part = jnp.dot(rotated, wts[j], preferred_element_type=F32)
                p[k, j] = part.reshape(4, 2, 8, COLS)
                p_copy(k, j).start()

            @pl.when(j > 0)
            def _():
                i = j - 1
                p_copy(k, i).wait_recv()
                q[k, i] = (p[k, i, :, c] + pr[k, i]).astype(BF16)
                for d in range(3):
                    q_copy(k, i, d).start()

            return carry

        lax.fori_loop(0, BLOCKS + 1, block, 0)

    def o_copy(k, j):
        return remote(r1.at[k, j], r1r.at[k, j], o_s.at[k, j], o_r.at[k, j], far)

    def gather(k):
        def block(j, carry):
            total = p[k, j, y, c] + pr[k, j, y]
            for d in range(3):
                q_copy(k, j, d).wait_recv()
                total = total + qr[k, j, d].astype(F32)
            if k < 2:
                r1[k, j] = total.astype(BF16)
                o_copy(k, j).start()
            else:
                o_copy(k - 2, j).wait_recv()
                acc[k - 2, j] = total + r1r[k - 2, j].astype(F32)
            return carry

        lax.fori_loop(0, BLOCKS, block, 0)

    def finish(s):
        square = jnp.zeros((8, 1), F32)
        for j in range(BLOCKS):
            lanes = slice(j * COLS, (j + 1) * COLS)
            new = (res[s, :, lanes].astype(F32) + acc[s, j] * BRANCH).astype(BF16)
            new_out[s, :, lanes] = new
            values = new.astype(F32)
            square = square + jnp.sum(values * values, axis=1, keepdims=True)
        factor = lax.rsqrt(square * (1.0 / D) + 1e-05)
        for j in range(BLOCKS):
            lanes = slice(j * COLS, (j + 1) * COLS)
            norm_out[s, :, lanes] = (new_out[s, :, lanes].astype(F32) * factor).astype(BF16)

    combine_far(0)
    combine_twin(0)
    multiply(0)
    combine_far(1)
    combine_twin(1)
    gather(0)
    multiply(1)
    combine_far(2)
    combine_twin(2)
    gather(1)
    multiply(2)
    combine_far(3)
    combine_twin(3)
    loads[5].wait()
    gather(2)
    finish(0)
    multiply(3)
    gather(3)
    finish(1)

    for k in range(CHUNKS):
        zin_copies[k].wait_send()
        v_copies[k].wait_send()
        for d in range(3):
            w_copies[k, d].wait_send()

    def drain(j, carry):
        for k in range(CHUNKS):
            p_copy(k, j).wait_send()
            for d in range(3):
                q_copy(k, j, d).wait_send()
            if k < 2:
                o_copy(k, j).wait_send()
        return carry

    lax.fori_loop(0, BLOCKS, drain, 0)


def local(hidden, signs, packed, group_scales, residual):
    table = jnp.asarray(np.kron(sylvester(LOCAL // 28), paley_table()), BF16)
    sem = pltpu.SemaphoreType.DMA
    outs = pl.pallas_call(
        kernel,
        out_shape=[jax.ShapeDtypeStruct((2, 8, D), BF16)] * 2,
        in_specs=[pl.BlockSpec(memory_space=pl.ANY)] * 6,
        out_specs=[pl.BlockSpec(memory_space=pltpu.VMEM)] * 2,
        scratch_shapes=[
            pltpu.VMEM((2, 4, 2, 2, 8, LOCAL), BF16),
            pltpu.VMEM((CHUNKS, 4, 2, 8, LOCAL), BF16),
            pltpu.VMEM((2, GROUPS, 128), jnp.int32),
            pltpu.VMEM((LOCAL, WORDS), jnp.int32),
            pltpu.VMEM((GROUPS, D), jnp.int32),
            pltpu.VMEM((2, 8, D), BF16),
            pltpu.VMEM((LOCAL, LOCAL), BF16),
            pltpu.VMEM((BLOCKS, LOCAL, COLS), BF16),
            pltpu.VMEM((CHUNKS, 4, 2, 8, LOCAL), F32),
            pltpu.VMEM((CHUNKS, 4, 2, 8, LOCAL), F32),
            pltpu.VMEM((CHUNKS, 4, 2, 8, LOCAL), BF16),
            pltpu.VMEM((CHUNKS, 3, 4, 2, 8, LOCAL), BF16),
            pltpu.VMEM((CHUNKS, BLOCKS, 4, 2, 8, COLS), F32),
            pltpu.VMEM((CHUNKS, BLOCKS, 4, 8, COLS), F32),
            pltpu.VMEM((CHUNKS, BLOCKS, 4, 8, COLS), BF16),
            pltpu.VMEM((CHUNKS, BLOCKS, 3, 8, COLS), BF16),
            pltpu.VMEM((2, BLOCKS, 8, COLS), BF16),
            pltpu.VMEM((2, BLOCKS, 8, COLS), BF16),
            pltpu.VMEM((2, BLOCKS, 8, COLS), F32),
            sem((6,)),
            sem((CHUNKS,)),
            sem((CHUNKS,)),
            sem,
            sem,
            sem((CHUNKS,)),
            sem((CHUNKS,)),
            sem((CHUNKS, 3)),
            sem((CHUNKS, 3)),
            sem((CHUNKS, BLOCKS)),
            sem((CHUNKS, BLOCKS)),
            sem((CHUNKS, BLOCKS, 3)),
            sem((CHUNKS, BLOCKS, 3)),
            sem((2, BLOCKS)),
            sem((2, BLOCKS)),
        ],
        compiler_params=pltpu.CompilerParams(
            collective_id=0, has_side_effects=True, vmem_limit_bytes=56 * 2**20
        ),
        name="rotated_down",
    )(
        hidden.reshape(2, 4, 2, 2, 8, LOCAL),
        signs.reshape(GROUPS, 128),
        packed,
        group_scales,
        residual.reshape(2, 8, D),
        table,
    )
    return tuple(out.reshape(16, D) for out in outs)


def solution(mesh):
    in_specs = (P("dp", "tensor"), P("tensor"), P("tensor", None), P("tensor", None), P(("dp", "tensor"), None))
    out_specs = (P(("dp", "tensor"), None), P(("dp", "tensor"), None))
    return jax.shard_map(local, mesh=mesh, in_specs=in_specs, out_specs=out_specs, check_vma=False)
```

```python
import functools
import math

import jax
import jax.numpy as jnp
import numpy as np
from jax import lax
from jax.experimental import pallas as pl
from jax.experimental.pallas import tpu as pltpu
from jax.sharding import PartitionSpec as P

FF = 14336
D = 4096
LOCAL = 896
WORDS = 512
GROUPS = 7
CHUNKS = 4
BLOCKS = 4
COLS = D // BLOCKS
MESH = pl.DeviceIdType.MESH
UNIT = 1.0 / math.sqrt(FF)
BRANCH = 1.0 / (45.0 * math.sqrt(FF))
F32 = jnp.float32
BF16 = jnp.bfloat16


def paley_table():
    offsets = (np.arange(13)[None, :] - np.arange(13)[:, None]) % 13
    residues = np.zeros(13)
    residues[np.arange(1, 13) ** 2 % 13] = 1.0
    quadratic = np.where(offsets == 0, 0.0, np.where(residues[offsets] > 0, 1.0, -1.0))
    conference = np.zeros((14, 14))
    conference[0, 1:] = 1.0
    conference[1:, 0] = 1.0
    conference[1:, 1:] = quadratic
    upper = np.array([[1.0, 1.0], [1.0, -1.0]])
    lower = np.array([[1.0, -1.0], [-1.0, -1.0]])
    return np.kron(conference, upper) + np.kron(np.eye(14), lower)


def sylvester(order):
    table = np.ones((1, 1))
    while table.shape[0] < order:
        table = np.kron(np.array([[1.0, 1.0], [1.0, -1.0]]), table)
    return table


def sign_of(bits):
    odd = lax.rem(bits + bits // 2, 2)
    return 1.0 - 2.0 * odd.astype(F32)


def kernel(
    hidden,
    signs,
    packed,
    scales,
    residual,
    table_hbm,
    new_out,
    norm_out,
    h,
    zin,
    sg,
    pk,
    sc,
    res,
    table,
    wts,
    v,
    vr,
    w,
    wr,
    p,
    pr,
    q,
    qr,
    r1,
    r1r,
    acc,
    local_sem,
    zin_s,
    zin_r,
    sg_s,
    sg_r,
    v_s,
    v_r,
    w_s,
    w_r,
    p_s,
    p_r,
    q_s,
    q_r,
    o_s,
    o_r,
):
    dp = lax.axis_index("dp")
    t = lax.axis_index("tensor")
    z = t // 8
    y = lax.rem(t // 2, 4)
    c = lax.rem(t, 2)

    def dev(zz, yy, cc):
        return (dp, zz * 8 + yy * 2 + cc)

    far = dev(1 - z, y, c)
    twin = dev(z, y, 1 - c)
    ring = [dev(z, lax.rem(y + d, 4), c) for d in (1, 2, 3)]

    loads = [
        pltpu.make_async_copy(hidden, h, local_sem.at[0]),
        pltpu.make_async_copy(signs, sg.at[0], local_sem.at[1]),
        pltpu.make_async_copy(packed, pk, local_sem.at[2]),
        pltpu.make_async_copy(scales, sc, local_sem.at[3]),
        pltpu.make_async_copy(table_hbm, table, local_sem.at[4]),
        pltpu.make_async_copy(residual, res, local_sem.at[5]),
    ]
    for load in loads:
        load.start()

    barrier = pltpu.get_barrier_semaphore()
    for peer in [far, twin] + ring:
        pl.semaphore_signal(barrier, 1, device_id=peer, device_id_type=MESH)
    pl.semaphore_wait(barrier, 5)

    def remote(src, dst, ss, rs, peer):
        return pltpu.make_async_remote_copy(
            src_ref=src, dst_ref=dst, send_sem=ss, recv_sem=rs, device_id=peer, device_id_type=MESH
        )

    loads[1].wait()
    sg_copy = remote(sg.at[0], sg.at[1], sg_s, sg_r, far)
    sg_copy.start()
    loads[0].wait()
    zin_copies = []
    for k in range(CHUNKS):
        half = z if k < 2 else 1 - z
        copy = remote(h.at[half, :, :, k % 2], zin.at[k], zin_s.at[k], zin_r.at[k], far)
        if k < 2:
            copy.start()
        zin_copies.append(copy)

    loads[2].wait()
    loads[3].wait()

    def dequantize(i, carry):
        rows = pl.ds(pl.multiple_of(i * 16, 16), 16)
        words = pk[rows, :] ^ jnp.int32(-2004318072)
        for k in range(8):
            codes = jnp.right_shift(jnp.left_shift(words, 28 - 4 * k), 28)
            scale = sc[pl.ds(i // 8, 1), k * WORDS : (k + 1) * WORDS]
            value = (codes.astype(F32) * scale.astype(F32)).astype(BF16)
            wts[k // 2, rows, (k % 2) * WORDS : (k % 2 + 1) * WORDS] = value
        return carry

    lax.fori_loop(0, LOCAL // 16, dequantize, 0)
    loads[4].wait()

    sg_copy.wait()
    flips = (2 * sg[...] - 1).astype(F32)
    own_flip = flips[0] * (1 - 2 * z).astype(F32)
    far_flip = flips[1]

    v_copies, w_copies, p_copies, q_copies, o_copies = {}, {}, {}, {}, {}

    def combine_far(k):
        half = 1 - z if k < 2 else z
        zin_copies[k].wait_recv()
        if k + 2 < CHUNKS:
            zin_copies[k + 2].start()
        for g in range(GROUPS):
            lanes = slice(g * 128, (g + 1) * 128)
            own = h[half, :, :, k % 2, :, lanes].astype(F32)
            other = zin[k, :, :, :, lanes].astype(F32)
            v[k, :, :, :, lanes] = own * own_flip[g : g + 1] + other * far_flip[g : g + 1]
        v_copies[k] = remote(v.at[k], vr.at[k], v_s.at[k], v_r.at[k], twin)
        v_copies[k].start()

    def combine_twin(k):
        v_copies[k].wait_recv()
        w[k] = (vr[k] + v[k] * (1 - 2 * c).astype(F32)).astype(BF16)
        for d in range(3):
            w_copies[k, d] = remote(w.at[k], wr.at[k, d], w_s.at[k, d], w_r.at[k, d], ring[d])
            w_copies[k, d].start()

    def p_copy(k, j):
        return remote(p.at[k, j, :, 1 - c], pr.at[k, j], p_s.at[k, j], p_r.at[k, j], twin)

    def q_copy(k, j, d):
        return remote(
            q.at[k, j, lax.rem(y + d + 1, 4)], qr.at[k, j, d], q_s.at[k, j, d], q_r.at[k, j, d], ring[d]
        )

    def pass_on(k, i):
        p_copy(k, i).wait_recv()
        q[k, i] = (p[k, i, :, c] + pr[k, i]).astype(BF16)
        for d in range(3):
            q_copy(k, i, d).start()

    def multiply(k, inline=0):
        for d in range(3):
            w_copies[k, d].wait_recv()
        u = w[k].astype(F32) * sign_of(y)
        for d in range(3):
            source = lax.rem(y + 3 - d, 4)
            u = u + wr[k, d].astype(F32) * sign_of(y & source)
        u = u.reshape(64, LOCAL).astype(BF16)
        rotated = (jnp.dot(u, table[...], preferred_element_type=F32) * UNIT).astype(BF16)

        def block(j, carry):
            @pl.when(j < BLOCKS)
            def _():
                part = jnp.dot(rotated, wts[j], preferred_element_type=F32)
                p[k, j] = part.reshape(4, 2, 8, COLS)
                p_copy(k, j).start()

            if inline:

                @pl.when(j > 0)
                def _():
                    pass_on(k, j - 1)

            return carry

        lax.fori_loop(0, BLOCKS + inline, block, 0)

    def reduce(k):
        def block(j, carry):
            pass_on(k, j)
            return carry

        lax.fori_loop(0, BLOCKS, block, 0)

    def o_copy(k, j):
        return remote(r1.at[k, j], r1r.at[k, j], o_s.at[k, j], o_r.at[k, j], far)

    def gather(k):
        def block(j, carry):
            total = p[k, j, y, c] + pr[k, j, y]
            for d in range(3):
                q_copy(k, j, d).wait_recv()
                total = total + qr[k, j, d].astype(F32)
            if k < 2:
                r1[k, j] = total.astype(BF16)
                o_copy(k, j).start()
            else:
                o_copy(k - 2, j).wait_recv()
                acc[k - 2, j] = total + r1r[k - 2, j].astype(F32)
            return carry

        lax.fori_loop(0, BLOCKS, block, 0)

    def finish(s):
        square = jnp.zeros((8, 1), F32)
        for j in range(BLOCKS):
            lanes = slice(j * COLS, (j + 1) * COLS)
            new = (res[s, :, lanes].astype(F32) + acc[s, j] * BRANCH).astype(BF16)
            new_out[s, :, lanes] = new
            values = new.astype(F32)
            square = square + jnp.sum(values * values, axis=1, keepdims=True)
        factor = lax.rsqrt(square * (1.0 / D) + 1e-05)
        for j in range(BLOCKS):
            lanes = slice(j * COLS, (j + 1) * COLS)
            norm_out[s, :, lanes] = (new_out[s, :, lanes].astype(F32) * factor).astype(BF16)

    combine_far(0)
    combine_twin(0)
    combine_far(1)
    combine_twin(1)
    multiply(0)
    reduce(0)
    combine_far(2)
    combine_twin(2)
    multiply(1)
    reduce(1)
    gather(0)
    combine_far(3)
    combine_twin(3)
    gather(1)
    multiply(2)
    reduce(2)
    multiply(3, 1)
    loads[5].wait()
    gather(2)
    finish(0)
    gather(3)
    finish(1)

    for k in range(CHUNKS):
        zin_copies[k].wait_send()
        v_copies[k].wait_send()
        for d in range(3):
            w_copies[k, d].wait_send()

    def drain(j, carry):
        for k in range(CHUNKS):
            p_copy(k, j).wait_send()
            for d in range(3):
                q_copy(k, j, d).wait_send()
            if k < 2:
                o_copy(k, j).wait_send()
        return carry

    lax.fori_loop(0, BLOCKS, drain, 0)


def local(hidden, signs, packed, group_scales, residual):
    table = jnp.asarray(np.kron(sylvester(LOCAL // 28), paley_table()), BF16)
    sem = pltpu.SemaphoreType.DMA
    outs = pl.pallas_call(
        kernel,
        out_shape=[jax.ShapeDtypeStruct((2, 8, D), BF16)] * 2,
        in_specs=[pl.BlockSpec(memory_space=pltpu.HBM)] * 6,
        out_specs=[pl.BlockSpec(memory_space=pltpu.VMEM)] * 2,
        scratch_shapes=[
            pltpu.VMEM((2, 4, 2, 2, 8, LOCAL), BF16),
            pltpu.VMEM((CHUNKS, 4, 2, 8, LOCAL), BF16),
            pltpu.VMEM((2, GROUPS, 128), jnp.int32),
            pltpu.VMEM((LOCAL, WORDS), jnp.int32),
            pltpu.VMEM((GROUPS, D), jnp.int32),
            pltpu.VMEM((2, 8, D), BF16),
            pltpu.VMEM((LOCAL, LOCAL), BF16),
            pltpu.VMEM((BLOCKS, LOCAL, COLS), BF16),
            pltpu.VMEM((CHUNKS, 4, 2, 8, LOCAL), F32),
            pltpu.VMEM((CHUNKS, 4, 2, 8, LOCAL), F32),
            pltpu.VMEM((CHUNKS, 4, 2, 8, LOCAL), BF16),
            pltpu.VMEM((CHUNKS, 3, 4, 2, 8, LOCAL), BF16),
            pltpu.VMEM((CHUNKS, BLOCKS, 4, 2, 8, COLS), F32),
            pltpu.VMEM((CHUNKS, BLOCKS, 4, 8, COLS), F32),
            pltpu.VMEM((CHUNKS, BLOCKS, 4, 8, COLS), BF16),
            pltpu.VMEM((CHUNKS, BLOCKS, 3, 8, COLS), BF16),
            pltpu.VMEM((2, BLOCKS, 8, COLS), BF16),
            pltpu.VMEM((2, BLOCKS, 8, COLS), BF16),
            pltpu.VMEM((2, BLOCKS, 8, COLS), F32),
            sem((6,)),
            sem((CHUNKS,)),
            sem((CHUNKS,)),
            sem,
            sem,
            sem((CHUNKS,)),
            sem((CHUNKS,)),
            sem((CHUNKS, 3)),
            sem((CHUNKS, 3)),
            sem((CHUNKS, BLOCKS)),
            sem((CHUNKS, BLOCKS)),
            sem((CHUNKS, BLOCKS, 3)),
            sem((CHUNKS, BLOCKS, 3)),
            sem((2, BLOCKS)),
            sem((2, BLOCKS)),
        ],
        compiler_params=pltpu.CompilerParams(
            collective_id=0, has_side_effects=True, vmem_limit_bytes=66500000
        ),
        name="rotated_down",
    )(
        hidden.reshape(2, 4, 2, 2, 8, LOCAL),
        signs.reshape(GROUPS, 128),
        packed,
        group_scales,
        residual.reshape(2, 8, D),
        table,
    )
    return tuple(out.reshape(16, D) for out in outs)


def solution(mesh):
    in_specs = (P("dp", "tensor"), P("tensor"), P("tensor", None), P("tensor", None), P(("dp", "tensor"), None))
    out_specs = (P(("dp", "tensor"), None), P(("dp", "tensor"), None))
    return jax.shard_map(local, mesh=mesh, in_specs=in_specs, out_specs=out_specs, check_vma=False)
```

```python
import functools
import math

import jax
import jax.numpy as jnp
import numpy as np
from jax import lax
from jax.experimental import pallas as pl
from jax.experimental.pallas import tpu as pltpu
from jax.sharding import PartitionSpec as P

FF = 14336
D = 4096
LOCAL = 896
WORDS = 512
GROUPS = 7
CHUNKS = 4
BLOCKS = 4
COLS = D // BLOCKS
MESH = pl.DeviceIdType.MESH
UNIT = 1.0 / math.sqrt(FF)
BRANCH = 1.0 / (45.0 * math.sqrt(FF))
F32 = jnp.float32
BF16 = jnp.bfloat16


def paley_table():
    offsets = (np.arange(13)[None, :] - np.arange(13)[:, None]) % 13
    residues = np.zeros(13)
    residues[np.arange(1, 13) ** 2 % 13] = 1.0
    quadratic = np.where(offsets == 0, 0.0, np.where(residues[offsets] > 0, 1.0, -1.0))
    conference = np.zeros((14, 14))
    conference[0, 1:] = 1.0
    conference[1:, 0] = 1.0
    conference[1:, 1:] = quadratic
    upper = np.array([[1.0, 1.0], [1.0, -1.0]])
    lower = np.array([[1.0, -1.0], [-1.0, -1.0]])
    return np.kron(conference, upper) + np.kron(np.eye(14), lower)


def sylvester(order):
    table = np.ones((1, 1))
    while table.shape[0] < order:
        table = np.kron(np.array([[1.0, 1.0], [1.0, -1.0]]), table)
    return table


def sign_of(bits):
    odd = lax.rem(bits + bits // 2, 2)
    return 1.0 - 2.0 * odd.astype(F32)


def kernel(
    hidden,
    signs,
    packed,
    scales,
    residual,
    table_hbm,
    new_out,
    norm_out,
    h,
    zin,
    sg,
    pk,
    sc,
    res,
    table,
    wts,
    v,
    vr,
    w,
    wr,
    half_rot,
    half_send,
    p,
    pr,
    q,
    qr,
    r1,
    r1r,
    acc,
    local_sem,
    zin_s,
    zin_r,
    sg_s,
    sg_r,
    v_s,
    v_r,
    w_s,
    w_r,
    p_s,
    p_r,
    q_s,
    q_r,
    o_s,
    o_r,
):
    dp = lax.axis_index("dp")
    t = lax.axis_index("tensor")
    z = t // 8
    y = lax.rem(t // 2, 4)
    c = lax.rem(t, 2)

    def dev(zz, yy, cc):
        return (dp, zz * 8 + yy * 2 + cc)

    far = dev(1 - z, y, c)
    twin = dev(z, y, 1 - c)
    ring = [dev(z, lax.rem(y + d, 4), c) for d in (1, 2, 3)]

    loads = [
        pltpu.make_async_copy(hidden, h, local_sem.at[0]),
        pltpu.make_async_copy(signs, sg.at[0], local_sem.at[1]),
        pltpu.make_async_copy(packed, pk, local_sem.at[2]),
        pltpu.make_async_copy(scales, sc, local_sem.at[3]),
        pltpu.make_async_copy(table_hbm, table, local_sem.at[4]),
        pltpu.make_async_copy(residual, res, local_sem.at[5]),
    ]
    barrier = pltpu.get_barrier_semaphore()
    for peer in [far, twin] + ring:
        pl.semaphore_signal(barrier, 1, device_id=peer, device_id_type=MESH)
    for load in loads:
        load.start()

    def remote(src, dst, ss, rs, peer):
        return pltpu.make_async_remote_copy(
            src_ref=src, dst_ref=dst, send_sem=ss, recv_sem=rs, device_id=peer, device_id_type=MESH
        )

    def dequantize(i, carry):
        rows = pl.ds(pl.multiple_of(i * 16, 16), 16)
        words = pk[rows, :] ^ jnp.int32(-2004318072)
        for k in range(8):
            codes = jnp.right_shift(jnp.left_shift(words, 28 - 4 * k), 28)
            scale = sc[pl.ds(i // 8, 1), k * WORDS : (k + 1) * WORDS]
            value = (codes.astype(F32) * scale.astype(F32)).astype(BF16)
            wts[k // 2, rows, (k % 2) * WORDS : (k % 2 + 1) * WORDS] = value
        return carry

    loads[1].wait()
    loads[0].wait()
    own_flip = (2 * sg[0] - 1).astype(F32)
    for half in range(2):
        for s in range(2):
            for g in range(GROUPS):
                lanes = slice(g * 128, (g + 1) * 128)
                own = h[half, :, :, s, :, lanes].astype(F32)
                v[half * 2 + s, :, :, :, lanes] = (own * own_flip[g : g + 1]).astype(BF16)
    loads[2].wait()
    loads[3].wait()

    @pl.when(z == 0)
    def _():
        lax.fori_loop(0, LOCAL // 16, dequantize, 0)

    pl.semaphore_wait(barrier, 5)

    sg_copy = remote(sg.at[0], sg.at[1], sg_s, sg_r, far)
    sg_copy.start()
    zin_copies = [
        remote(
            h.at[z, :, :, 0] if k == 0 else half_send.at[k - 1], zin.at[k], zin_s.at[k], zin_r.at[k], far
        )
        for k in range(CHUNKS)
    ]
    zin_copies[0].start()

    sets = [z * 2 + 1, (1 - z) * 2, (1 - z) * 2 + 1, z * 2]
    v_copies, w_copies = {}, {}
    for i in range(5):
        source = v.at[sets[i]] if i < 4 else v.at[4]
        v_copies[i] = remote(source, vr.at[i], v_s.at[i], v_r.at[i], twin)
        for d in range(3):
            w_copies[i, d] = remote(w.at[i], wr.at[i, d], w_s.at[i, d], w_r.at[i, d], ring[d])
    for i in range(4):
        v_copies[i].start()

    def spread(i):
        v_copies[i].wait_recv()
        own = v[sets[i]] if i < 4 else v[4]
        twin_sign = (1 - 2 * c).astype(F32)
        w[i] = (vr[i].astype(F32) + own.astype(F32) * twin_sign).astype(BF16)
        for d in range(3):
            w_copies[i, d].start()

    def absorb(i):
        for d in range(3):
            w_copies[i, d].wait_recv()
        u = w[i].astype(F32) * sign_of(y)
        for d in range(3):
            source = lax.rem(y + 3 - d, 4)
            u = u + wr[i, d].astype(F32) * sign_of(y & source)
        u = u.reshape(64, LOCAL).astype(BF16)
        return jnp.dot(u, table[...], preferred_element_type=F32)

    def rotate(i):
        mine = absorb(i)
        half_rot[sets[i]] = mine
        if i < 3:
            half_send[i] = mine.astype(BF16).reshape(4, 2, 8, LOCAL)

    def receive(k):
        zin_copies[k].wait_recv()
        if k + 2 < CHUNKS:
            zin_copies[k + 2].start()

    def spread_far():
        sg_copy.wait()
        far_flip = (2 * sg[1] - 1).astype(F32)
        for g in range(GROUPS):
            lanes = slice(g * 128, (g + 1) * 128)
            other = zin[0, :, :, :, lanes].astype(F32)
            v[4, :, :, :, lanes] = (other * far_flip[g : g + 1]).astype(BF16)
        v_copies[4].start()

    def p_copy(k, j):
        return remote(p.at[k, j, :, 1 - c], pr.at[k, j], p_s.at[k, j], p_r.at[k, j], twin)

    def q_copy(k, j, d):
        return remote(
            q.at[k, j, lax.rem(y + d + 1, 4)], qr.at[k, j, d], q_s.at[k, j, d], q_r.at[k, j, d], ring[d]
        )

    def o_copy(k, j):
        return remote(r1.at[k, j], r1r.at[k, j], o_s.at[k, j], o_r.at[k, j], far)

    def multiply(k):
        far_part = absorb(4) if k == 0 else zin[k].astype(F32).reshape(64, LOCAL)
        half = 1 - z if k < 2 else z
        own_part = half_rot[half * 2 + k % 2] * (1 - 2 * z).astype(F32)
        rotated = ((far_part + own_part) * UNIT).astype(BF16)

        def block(j, carry):
            part = jnp.dot(rotated, wts[j], preferred_element_type=F32)
            p[k, j] = part.reshape(4, 2, 8, COLS)
            p_copy(k, j).start()
            return carry

        lax.fori_loop(0, BLOCKS, block, 0)

    def reduce(k):
        def block(j, carry):
            p_copy(k, j).wait_recv()
            q[k, j] = (p[k, j, :, c] + pr[k, j]).astype(BF16)
            for d in range(3):
                q_copy(k, j, d).start()
            return carry

        lax.fori_loop(0, BLOCKS, block, 0)

    def gather(k):
        def block(j, carry):
            total = p[k, j, y, c] + pr[k, j, y]
            for d in range(3):
                q_copy(k, j, d).wait_recv()
                total = total + qr[k, j, d].astype(F32)
            if k < 2:
                r1[k, j] = total.astype(BF16)
                o_copy(k, j).start()
            else:
                o_copy(k - 2, j).wait_recv()
                acc[k - 2, j] = total + r1r[k - 2, j].astype(F32)
            return carry

        lax.fori_loop(0, BLOCKS, block, 0)

    def finish(s):
        square = jnp.zeros((8, 1), F32)
        for j in range(BLOCKS):
            lanes = slice(j * COLS, (j + 1) * COLS)
            new = (res[s, :, lanes].astype(F32) + acc[s, j] * BRANCH).astype(BF16)
            new_out[s, :, lanes] = new
            values = new.astype(F32)
            square = square + jnp.sum(values * values, axis=1, keepdims=True)
        factor = lax.rsqrt(square * (1.0 / D) + 1e-05)
        for j in range(BLOCKS):
            lanes = slice(j * COLS, (j + 1) * COLS)
            norm_out[s, :, lanes] = (new_out[s, :, lanes].astype(F32) * factor).astype(BF16)

    spread(0)
    spread(1)
    spread(2)
    spread(3)

    @pl.when(z == 1)
    def _():
        lax.fori_loop(0, LOCAL // 16, dequantize, 0)

    loads[4].wait()
    rotate(0)
    zin_copies[1].start()
    rotate(1)
    rotate(2)
    rotate(3)
    receive(0)
    spread_far()
    spread(4)
    multiply(0)
    reduce(0)
    receive(1)
    multiply(1)
    reduce(1)
    gather(0)
    receive(2)
    multiply(2)
    reduce(2)
    gather(1)
    receive(3)
    multiply(3)
    reduce(3)
    loads[5].wait()
    gather(2)
    finish(0)
    gather(3)
    finish(1)

    for k in range(CHUNKS):
        zin_copies[k].wait_send()
    for i in range(5):
        v_copies[i].wait_send()
        for d in range(3):
            w_copies[i, d].wait_send()

    def drain(j, carry):
        for k in range(CHUNKS):
            p_copy(k, j).wait_send()
            for d in range(3):
                q_copy(k, j, d).wait_send()
            if k < 2:
                o_copy(k, j).wait_send()
        return carry

    lax.fori_loop(0, BLOCKS, drain, 0)


def local(hidden, signs, packed, group_scales, residual):
    table = jnp.asarray(np.kron(sylvester(LOCAL // 28), paley_table()), BF16)
    sem = pltpu.SemaphoreType.DMA
    outs = pl.pallas_call(
        kernel,
        out_shape=[jax.ShapeDtypeStruct((2, 8, D), BF16)] * 2,
        in_specs=[pl.BlockSpec(memory_space=pltpu.HBM)] * 6,
        out_specs=[pl.BlockSpec(memory_space=pltpu.VMEM)] * 2,
        scratch_shapes=[
            pltpu.VMEM((2, 4, 2, 2, 8, LOCAL), BF16),
            pltpu.VMEM((CHUNKS, 4, 2, 8, LOCAL), BF16),
            pltpu.VMEM((2, GROUPS, 128), jnp.int32),
            pltpu.VMEM((LOCAL, WORDS), jnp.int32),
            pltpu.VMEM((GROUPS, D), jnp.int32),
            pltpu.VMEM((2, 8, D), BF16),
            pltpu.VMEM((LOCAL, LOCAL), BF16),
            pltpu.VMEM((BLOCKS, LOCAL, COLS), BF16),
            pltpu.VMEM((5, 4, 2, 8, LOCAL), BF16),
            pltpu.VMEM((5, 4, 2, 8, LOCAL), BF16),
            pltpu.VMEM((5, 4, 2, 8, LOCAL), BF16),
            pltpu.VMEM((5, 3, 4, 2, 8, LOCAL), BF16),
            pltpu.VMEM((4, 64, LOCAL), F32),
            pltpu.VMEM((3, 4, 2, 8, LOCAL), BF16),
            pltpu.VMEM((CHUNKS, BLOCKS, 4, 2, 8, COLS), F32),
            pltpu.VMEM((CHUNKS, BLOCKS, 4, 8, COLS), F32),
            pltpu.VMEM((CHUNKS, BLOCKS, 4, 8, COLS), BF16),
            pltpu.VMEM((CHUNKS, BLOCKS, 3, 8, COLS), BF16),
            pltpu.VMEM((2, BLOCKS, 8, COLS), BF16),
            pltpu.VMEM((2, BLOCKS, 8, COLS), BF16),
            pltpu.VMEM((2, BLOCKS, 8, COLS), F32),
            sem((6,)),
            sem((CHUNKS,)),
            sem((CHUNKS,)),
            sem,
            sem,
            sem((5,)),
            sem((5,)),
            sem((5, 3)),
            sem((5, 3)),
            sem((CHUNKS, BLOCKS)),
            sem((CHUNKS, BLOCKS)),
            sem((CHUNKS, BLOCKS, 3)),
            sem((CHUNKS, BLOCKS, 3)),
            sem((2, BLOCKS)),
            sem((2, BLOCKS)),
        ],
        compiler_params=pltpu.CompilerParams(
            collective_id=0, has_side_effects=True, vmem_limit_bytes=66500000
        ),
        name="rotated_down",
    )(
        hidden.reshape(2, 4, 2, 2, 8, LOCAL),
        signs.reshape(GROUPS, 128),
        packed,
        group_scales,
        residual.reshape(2, 8, D),
        table,
    )
    return tuple(out.reshape(16, D) for out in outs)


def solution(mesh):
    in_specs = (P("dp", "tensor"), P("tensor"), P("tensor", None), P("tensor", None), P(("dp", "tensor"), None))
    out_specs = (P(("dp", "tensor"), None), P(("dp", "tensor"), None))
    return jax.shard_map(local, mesh=mesh, in_specs=in_specs, out_specs=out_specs, check_vma=False)
```

```python
import functools
import math

import jax
import jax.numpy as jnp
import numpy as np
from jax import lax
from jax.experimental import pallas as pl
from jax.experimental.pallas import tpu as pltpu
from jax.sharding import PartitionSpec as P

FF = 14336
D = 4096
LOCAL = 896
WORDS = 512
GROUPS = 7
CHUNKS = 4
BLOCKS = 4
COLS = D // BLOCKS
MESH = pl.DeviceIdType.MESH
UNIT = 1.0 / math.sqrt(FF)
BRANCH = 1.0 / (45.0 * math.sqrt(FF))
F32 = jnp.float32
BF16 = jnp.bfloat16


def paley_table():
    offsets = (np.arange(13)[None, :] - np.arange(13)[:, None]) % 13
    residues = np.zeros(13)
    residues[np.arange(1, 13) ** 2 % 13] = 1.0
    quadratic = np.where(offsets == 0, 0.0, np.where(residues[offsets] > 0, 1.0, -1.0))
    conference = np.zeros((14, 14))
    conference[0, 1:] = 1.0
    conference[1:, 0] = 1.0
    conference[1:, 1:] = quadratic
    upper = np.array([[1.0, 1.0], [1.0, -1.0]])
    lower = np.array([[1.0, -1.0], [-1.0, -1.0]])
    return np.kron(conference, upper) + np.kron(np.eye(14), lower)


def sylvester(order):
    table = np.ones((1, 1))
    while table.shape[0] < order:
        table = np.kron(np.array([[1.0, 1.0], [1.0, -1.0]]), table)
    return table


def sign_of(bits):
    odd = lax.rem(bits + bits // 2, 2)
    return 1.0 - 2.0 * odd.astype(F32)


def kernel(
    hidden,
    signs,
    packed,
    scales,
    residual,
    table_hbm,
    new_out,
    norm_out,
    h,
    zin,
    sg,
    pk,
    sc,
    res,
    table,
    wts,
    v,
    vr,
    w,
    wr,
    ub,
    ur,
    half_rot,
    half_send,
    p,
    pr,
    q,
    qr,
    r1,
    r1r,
    acc,
    local_sem,
    zin_s,
    zin_r,
    sg_s,
    sg_r,
    v_s,
    v_r,
    w_s,
    w_r,
    u_s,
    u_r,
    p_s,
    p_r,
    q_s,
    q_r,
    o_s,
    o_r,
):
    dp = lax.axis_index("dp")
    t = lax.axis_index("tensor")
    z = t // 8
    y = lax.rem(t // 2, 4)
    c = lax.rem(t, 2)

    def dev(zz, yy, cc):
        return (dp, zz * 8 + yy * 2 + cc)

    far = dev(1 - z, y, c)
    twin = dev(z, y, 1 - c)
    ring = [dev(z, lax.rem(y + d, 4), c) for d in (1, 2, 3)]

    loads = [
        pltpu.make_async_copy(hidden, h, local_sem.at[0]),
        pltpu.make_async_copy(signs, sg.at[0], local_sem.at[1]),
        pltpu.make_async_copy(packed, pk, local_sem.at[2]),
        pltpu.make_async_copy(scales, sc, local_sem.at[3]),
        pltpu.make_async_copy(table_hbm, table, local_sem.at[4]),
        pltpu.make_async_copy(residual, res, local_sem.at[5]),
    ]
    barrier = pltpu.get_barrier_semaphore()
    for peer in [far, twin] + ring:
        pl.semaphore_signal(barrier, 1, device_id=peer, device_id_type=MESH)
    for load in loads:
        load.start()

    def remote(src, dst, ss, rs, peer):
        return pltpu.make_async_remote_copy(
            src_ref=src, dst_ref=dst, send_sem=ss, recv_sem=rs, device_id=peer, device_id_type=MESH
        )

    def dequantize(i, carry):
        rows = pl.ds(pl.multiple_of(i * 16, 16), 16)
        words = pk[rows, :] ^ jnp.int32(-2004318072)
        for k in range(8):
            codes = jnp.right_shift(jnp.left_shift(words, 28 - 4 * k), 28)
            scale = sc[pl.ds(i // 8, 1), k * WORDS : (k + 1) * WORDS]
            value = (codes.astype(F32) * scale.astype(F32)).astype(BF16)
            wts[k // 2, rows, (k % 2) * WORDS : (k % 2 + 1) * WORDS] = value
        return carry

    loads[1].wait()
    loads[0].wait()
    own_flip = (2 * sg[0] - 1).astype(F32)
    for half in range(2):
        for s in range(2):
            for g in range(GROUPS):
                lanes = slice(g * 128, (g + 1) * 128)
                own = h[half, :, :, s, :, lanes].astype(F32)
                v[half * 2 + s, :, :, :, lanes] = (own * own_flip[g : g + 1]).astype(BF16)
    loads[2].wait()
    loads[3].wait()

    @pl.when(z == 0)
    def _():
        lax.fori_loop(0, LOCAL // 16, dequantize, 0)

    pl.semaphore_wait(barrier, 5)

    sg_copy = remote(sg.at[0], sg.at[1], sg_s, sg_r, far)
    sg_copy.start()
    zin_copies = [
        remote(
            h.at[z, :, :, 0] if k == 0 else half_send.at[k - 1], zin.at[k], zin_s.at[k], zin_r.at[k], far
        )
        for k in range(CHUNKS)
    ]
    zin_copies[0].start()

    sets = [z * 2 + 1, (1 - z) * 2, (1 - z) * 2 + 1, z * 2]
    v_copies, w_copies, u_copies = {}, {}, {}
    for i in range(5):
        source = v.at[sets[i]] if i < 4 else v.at[4]
        v_copies[i] = remote(source, vr.at[i], v_s.at[i], v_r.at[i], twin)
        for d in range(3):
            block = w.at[i, lax.rem(y + d + 1, 4)]
            w_copies[i, d] = remote(block, wr.at[i, d], w_s.at[i, d], w_r.at[i, d], ring[d])
            u_copies[i, d] = remote(ub.at[i, d], ur.at[i, y], u_s.at[i, d], u_r.at[i, d], ring[d])
    for i in range(4):
        v_copies[i].start()

    def spread(i):
        v_copies[i].wait_recv()
        own = v[sets[i]] if i < 4 else v[4]
        twin_sign = (1 - 2 * c).astype(F32)
        w[i] = (vr[i].astype(F32) + own.astype(F32) * twin_sign).astype(BF16)
        for d in range(3):
            w_copies[i, d].start()

    def turn(i):
        parts = [w[i, y].astype(F32)]
        for d in range(3):
            w_copies[i, d].wait_recv()
            parts.append(wr[i, d].astype(F32))
        for e in (1, 2, 3, 0):
            target = lax.rem(y + e, 4)
            u = sum(part * sign_of(target & lax.rem(y + 4 - d, 4)) for d, part in enumerate(parts))
            if e:
                ub[i, e - 1] = u.astype(BF16)
                u_copies[i, e - 1].start()
            else:
                ur[i, y] = u.astype(BF16)

    def absorb(i):
        for d in range(3):
            u_copies[i, d].wait_recv()
        return jnp.dot(ur[i].reshape(64, LOCAL), table[...], preferred_element_type=F32)

    def rotate(i):
        mine = absorb(i)
        half_rot[sets[i]] = mine
        if i < 3:
            half_send[i] = mine.astype(BF16).reshape(4, 2, 8, LOCAL)

    def receive(k):
        zin_copies[k].wait_recv()

    def spread_far():
        sg_copy.wait()
        far_flip = (2 * sg[1] - 1).astype(F32)
        for g in range(GROUPS):
            lanes = slice(g * 128, (g + 1) * 128)
            other = zin[0, :, :, :, lanes].astype(F32)
            v[4, :, :, :, lanes] = (other * far_flip[g : g + 1]).astype(BF16)
        v_copies[4].start()

    def p_copy(k, j):
        return remote(p.at[k, j, :, 1 - c], pr.at[k, j], p_s.at[k, j], p_r.at[k, j], twin)

    def q_copy(k, j, d):
        return remote(
            q.at[k, j, lax.rem(y + d + 1, 4)], qr.at[k, j, d], q_s.at[k, j, d], q_r.at[k, j, d], ring[d]
        )

    def o_copy(k, j):
        return remote(r1.at[k, j], r1r.at[k, j], o_s.at[k, j], o_r.at[k, j], far)

    def multiply(k):
        far_part = absorb(4) if k == 0 else zin[k].astype(F32).reshape(64, LOCAL)
        half = 1 - z if k < 2 else z
        own_part = half_rot[half * 2 + k % 2] * (1 - 2 * z).astype(F32)
        rotated = ((far_part + own_part) * UNIT).astype(BF16)

        def block(j, carry):
            part = jnp.dot(rotated, wts[j], preferred_element_type=F32)
            p[k, j] = part.reshape(4, 2, 8, COLS)
            p_copy(k, j).start()
            return carry

        lax.fori_loop(0, BLOCKS, block, 0)

    def reduce(k):
        def block(j, carry):
            p_copy(k, j).wait_recv()
            q[k, j] = (p[k, j, :, c] + pr[k, j]).astype(BF16)
            for d in range(3):
                q_copy(k, j, d).start()
            return carry

        lax.fori_loop(0, BLOCKS, block, 0)

    def gather(k):
        def block(j, carry):
            total = p[k, j, y, c] + pr[k, j, y]
            for d in range(3):
                q_copy(k, j, d).wait_recv()
                total = total + qr[k, j, d].astype(F32)
            if k < 2:
                r1[k, j] = total.astype(BF16)
                o_copy(k, j).start()
            else:
                o_copy(k - 2, j).wait_recv()
                acc[k - 2, j] = total + r1r[k - 2, j].astype(F32)
            return carry

        lax.fori_loop(0, BLOCKS, block, 0)

    def finish(s):
        square = jnp.zeros((8, 1), F32)
        for j in range(BLOCKS):
            lanes = slice(j * COLS, (j + 1) * COLS)
            new = (res[s, :, lanes].astype(F32) + acc[s, j] * BRANCH).astype(BF16)
            new_out[s, :, lanes] = new
            values = new.astype(F32)
            square = square + jnp.sum(values * values, axis=1, keepdims=True)
        factor = lax.rsqrt(square * (1.0 / D) + 1e-05)
        for j in range(BLOCKS):
            lanes = slice(j * COLS, (j + 1) * COLS)
            norm_out[s, :, lanes] = (new_out[s, :, lanes].astype(F32) * factor).astype(BF16)

    spread(0)
    spread(1)
    spread(2)
    spread(3)

    @pl.when(z == 1)
    def _():
        lax.fori_loop(0, LOCAL // 16, dequantize, 0)

    turn(0)
    turn(1)
    turn(2)
    loads[4].wait()
    rotate(0)
    zin_copies[1].start()
    turn(3)
    rotate(1)
    rotate(2)
    rotate(3)
    receive(0)
    zin_copies[2].start()
    spread_far()
    spread(4)
    turn(4)
    zin_copies[3].start()
    multiply(0)
    reduce(0)
    receive(1)
    multiply(1)
    reduce(1)
    receive(2)
    multiply(2)
    reduce(2)
    gather(0)
    receive(3)
    gather(1)
    multiply(3)
    reduce(3)
    loads[5].wait()
    gather(2)
    finish(0)
    gather(3)
    finish(1)

    for k in range(CHUNKS):
        zin_copies[k].wait_send()
    for i in range(5):
        v_copies[i].wait_send()
        for d in range(3):
            w_copies[i, d].wait_send()
            u_copies[i, d].wait_send()

    def drain(j, carry):
        for k in range(CHUNKS):
            p_copy(k, j).wait_send()
            for d in range(3):
                q_copy(k, j, d).wait_send()
            if k < 2:
                o_copy(k, j).wait_send()
        return carry

    lax.fori_loop(0, BLOCKS, drain, 0)


def local(hidden, signs, packed, group_scales, residual):
    table = jnp.asarray(np.kron(sylvester(LOCAL // 28), paley_table()), BF16)
    sem = pltpu.SemaphoreType.DMA
    outs = pl.pallas_call(
        kernel,
        out_shape=[jax.ShapeDtypeStruct((2, 8, D), BF16)] * 2,
        in_specs=[pl.BlockSpec(memory_space=pltpu.HBM)] * 6,
        out_specs=[pl.BlockSpec(memory_space=pltpu.VMEM)] * 2,
        scratch_shapes=[
            pltpu.VMEM((2, 4, 2, 2, 8, LOCAL), BF16),
            pltpu.VMEM((CHUNKS, 4, 2, 8, LOCAL), BF16),
            pltpu.VMEM((2, GROUPS, 128), jnp.int32),
            pltpu.VMEM((LOCAL, WORDS), jnp.int32),
            pltpu.VMEM((GROUPS, D), jnp.int32),
            pltpu.VMEM((2, 8, D), BF16),
            pltpu.VMEM((LOCAL, LOCAL), BF16),
            pltpu.VMEM((BLOCKS, LOCAL, COLS), BF16),
            pltpu.VMEM((5, 4, 2, 8, LOCAL), BF16),
            pltpu.VMEM((5, 4, 2, 8, LOCAL), BF16),
            pltpu.VMEM((5, 4, 2, 8, LOCAL), BF16),
            pltpu.VMEM((5, 3, 2, 8, LOCAL), BF16),
            pltpu.VMEM((5, 3, 2, 8, LOCAL), BF16),
            pltpu.VMEM((5, 4, 2, 8, LOCAL), BF16),
            pltpu.VMEM((4, 64, LOCAL), F32),
            pltpu.VMEM((3, 4, 2, 8, LOCAL), BF16),
            pltpu.VMEM((CHUNKS, BLOCKS, 4, 2, 8, COLS), F32),
            pltpu.VMEM((CHUNKS, BLOCKS, 4, 8, COLS), F32),
            pltpu.VMEM((CHUNKS, BLOCKS, 4, 8, COLS), BF16),
            pltpu.VMEM((CHUNKS, BLOCKS, 3, 8, COLS), BF16),
            pltpu.VMEM((2, BLOCKS, 8, COLS), BF16),
            pltpu.VMEM((2, BLOCKS, 8, COLS), BF16),
            pltpu.VMEM((2, BLOCKS, 8, COLS), F32),
            sem((6,)),
            sem((CHUNKS,)),
            sem((CHUNKS,)),
            sem,
            sem,
            sem((5,)),
            sem((5,)),
            sem((5, 3)),
            sem((5, 3)),
            sem((5, 3)),
            sem((5, 3)),
            sem((CHUNKS, BLOCKS)),
            sem((CHUNKS, BLOCKS)),
            sem((CHUNKS, BLOCKS, 3)),
            sem((CHUNKS, BLOCKS, 3)),
            sem((2, BLOCKS)),
            sem((2, BLOCKS)),
        ],
        compiler_params=pltpu.CompilerParams(
            collective_id=0, has_side_effects=True, vmem_limit_bytes=56180000
        ),
        name="rotated_down",
    )(
        hidden.reshape(2, 4, 2, 2, 8, LOCAL),
        signs.reshape(GROUPS, 128),
        packed,
        group_scales,
        residual.reshape(2, 8, D),
        table,
    )
    return tuple(out.reshape(16, D) for out in outs)


def solution(mesh):
    in_specs = (P("dp", "tensor"), P("tensor"), P("tensor", None), P("tensor", None), P(("dp", "tensor"), None))
    out_specs = (P(("dp", "tensor"), None), P(("dp", "tensor"), None))
    return jax.shard_map(local, mesh=mesh, in_specs=in_specs, out_specs=out_specs, check_vma=False)
```

```python
import functools
import math

import jax
import jax.numpy as jnp
import numpy as np
from jax import lax
from jax.experimental import pallas as pl
from jax.experimental.pallas import tpu as pltpu
from jax.sharding import PartitionSpec as P

FF = 14336
D = 4096
LOCAL = 896
WORDS = 512
GROUPS = 7
CHUNKS = 4
BLOCKS = 4
COLS = D // BLOCKS
MESH = pl.DeviceIdType.MESH
UNIT = 1.0 / math.sqrt(FF)
BRANCH = 1.0 / (45.0 * math.sqrt(FF))
F32 = jnp.float32
BF16 = jnp.bfloat16


def paley_table():
    offsets = (np.arange(13)[None, :] - np.arange(13)[:, None]) % 13
    residues = np.zeros(13)
    residues[np.arange(1, 13) ** 2 % 13] = 1.0
    quadratic = np.where(offsets == 0, 0.0, np.where(residues[offsets] > 0, 1.0, -1.0))
    conference = np.zeros((14, 14))
    conference[0, 1:] = 1.0
    conference[1:, 0] = 1.0
    conference[1:, 1:] = quadratic
    upper = np.array([[1.0, 1.0], [1.0, -1.0]])
    lower = np.array([[1.0, -1.0], [-1.0, -1.0]])
    return np.kron(conference, upper) + np.kron(np.eye(14), lower)


def sylvester(order):
    table = np.ones((1, 1))
    while table.shape[0] < order:
        table = np.kron(np.array([[1.0, 1.0], [1.0, -1.0]]), table)
    return table


def sign_of(bits):
    odd = lax.rem(bits + bits // 2, 2)
    return 1.0 - 2.0 * odd.astype(F32)


def kernel(
    hidden,
    signs,
    packed,
    scales,
    residual,
    table_hbm,
    new_out,
    norm_out,
    h,
    zin,
    sg,
    pk,
    sc,
    res,
    table,
    wts,
    v,
    vr,
    w,
    wr,
    ub,
    ur,
    half_rot,
    half_send,
    p,
    pr,
    q,
    qr,
    r1,
    r1r,
    acc,
    local_sem,
    zin_s,
    zin_r,
    sg_s,
    sg_r,
    v_s,
    v_r,
    w_s,
    w_r,
    u_s,
    u_r,
    p_s,
    p_r,
    q_s,
    q_r,
    o_s,
    o_r,
):
    dp = lax.axis_index("dp")
    t = lax.axis_index("tensor")
    z = t // 8
    y = lax.rem(t // 2, 4)
    c = lax.rem(t, 2)

    def dev(zz, yy, cc):
        return (dp, zz * 8 + yy * 2 + cc)

    far = dev(1 - z, y, c)
    twin = dev(z, y, 1 - c)
    ring = [dev(z, lax.rem(y + d, 4), c) for d in (1, 2, 3)]

    loads = [
        pltpu.make_async_copy(hidden, h, local_sem.at[0]),
        pltpu.make_async_copy(signs, sg.at[0], local_sem.at[1]),
        pltpu.make_async_copy(packed, pk, local_sem.at[2]),
        pltpu.make_async_copy(scales, sc, local_sem.at[3]),
        pltpu.make_async_copy(table_hbm, table, local_sem.at[4]),
        pltpu.make_async_copy(residual, res, local_sem.at[5]),
    ]
    barrier = pltpu.get_barrier_semaphore()
    for peer in [far, twin] + ring:
        pl.semaphore_signal(barrier, 1, device_id=peer, device_id_type=MESH)
    for load in loads:
        load.start()

    def remote(src, dst, ss, rs, peer):
        return pltpu.make_async_remote_copy(
            src_ref=src, dst_ref=dst, send_sem=ss, recv_sem=rs, device_id=peer, device_id_type=MESH
        )

    def await_bytes(ref, semaphore):
        pltpu.make_async_copy(ref, ref, semaphore).wait()

    def dequantize(i, carry):
        rows = pl.ds(pl.multiple_of(i * 16, 16), 16)
        words = pk[rows, :] ^ jnp.int32(-2004318072)
        for k in range(8):
            codes = jnp.right_shift(jnp.left_shift(words, 28 - 4 * k), 28)
            scale = sc[pl.ds(i // 8, 1), k * WORDS : (k + 1) * WORDS]
            value = (codes.astype(F32) * scale.astype(F32)).astype(BF16)
            wts[k // 2, rows, (k % 2) * WORDS : (k % 2 + 1) * WORDS] = value
        return carry

    loads[1].wait()
    loads[0].wait()
    own_flip = (2 * sg[0] - 1).astype(F32)
    for half in range(2):
        for s in range(2):
            for g in range(GROUPS):
                lanes = slice(g * 128, (g + 1) * 128)
                own = h[half, :, :, s, :, lanes].astype(F32)
                v[half * 2 + s, :, :, :, lanes] = (own * own_flip[g : g + 1]).astype(BF16)
    loads[2].wait()
    loads[3].wait()

    @pl.when(z == 0)
    def _():
        lax.fori_loop(0, LOCAL // 16, dequantize, 0)

    pl.semaphore_wait(barrier, 5)

    sg_copy = remote(sg.at[0], sg.at[1], sg_s, sg_r, far)
    sg_copy.start()
    zin_copies = [
        remote(
            h.at[z, :, :, 0] if k == 0 else half_send.at[k - 1], zin.at[k], zin_s, zin_r.at[k], far
        )
        for k in range(CHUNKS)
    ]
    zin_copies[0].start()

    sets = [z * 2 + 1, (1 - z) * 2, (1 - z) * 2 + 1, z * 2]
    v_copies, w_copies, u_copies = {}, {}, {}
    for i in range(5):
        source = v.at[sets[i]] if i < 4 else v.at[4]
        v_copies[i] = remote(source, vr.at[i], v_s, v_r.at[i], twin)
        for d in range(3):
            block = w.at[i, lax.rem(y + d + 1, 4)]
            w_copies[i, d] = remote(block, wr.at[i, d], w_s, w_r.at[i], ring[d])
            u_copies[i, d] = remote(ub.at[i, d], ur.at[i, y], u_s, u_r.at[i], ring[d])
    for i in range(4):
        v_copies[i].start()

    def spread(i):
        v_copies[i].wait_recv()
        own = v[sets[i]] if i < 4 else v[4]
        twin_sign = (1 - 2 * c).astype(F32)
        w[i] = (vr[i].astype(F32) + own.astype(F32) * twin_sign).astype(BF16)
        for d in range(3):
            w_copies[i, d].start()

    def turn(i):
        parts = [w[i, y].astype(F32)]
        await_bytes(wr.at[i], w_r.at[i])
        for d in range(3):
            parts.append(wr[i, d].astype(F32))
        for e in (1, 2, 3, 0):
            target = lax.rem(y + e, 4)
            u = sum(part * sign_of(target & lax.rem(y + 4 - d, 4)) for d, part in enumerate(parts))
            if e:
                ub[i, e - 1] = u.astype(BF16)
                u_copies[i, e - 1].start()
            else:
                ur[i, y] = u.astype(BF16)

    def absorb(i):
        await_bytes(ub.at[i], u_r.at[i])
        return jnp.dot(ur[i].reshape(64, LOCAL), table[...], preferred_element_type=F32)

    def rotate(i):
        mine = absorb(i)
        half_rot[sets[i]] = mine
        if i < 3:
            half_send[i] = mine.astype(BF16).reshape(4, 2, 8, LOCAL)

    def receive(k):
        zin_copies[k].wait_recv()

    def spread_far():
        sg_copy.wait()
        far_flip = (2 * sg[1] - 1).astype(F32)
        for g in range(GROUPS):
            lanes = slice(g * 128, (g + 1) * 128)
            other = zin[0, :, :, :, lanes].astype(F32)
            v[4, :, :, :, lanes] = (other * far_flip[g : g + 1]).astype(BF16)
        v_copies[4].start()

    def p_copy(k, j):
        return remote(p.at[k, j, :, 1 - c], pr.at[k, j], p_s, p_r.at[k, j], twin)

    def q_copy(k, j, d):
        return remote(
            q.at[k, j, lax.rem(y + d + 1, 4)], qr.at[k, j, d], q_s, q_r.at[k, j], ring[d]
        )

    def o_copy(k, j):
        return remote(r1.at[k, j], r1r.at[k, j], o_s, o_r.at[k], far)

    def multiply(k):
        far_part = absorb(4) if k == 0 else zin[k].astype(F32).reshape(64, LOCAL)
        half = 1 - z if k < 2 else z
        own_part = half_rot[half * 2 + k % 2] * (1 - 2 * z).astype(F32)
        rotated = ((far_part + own_part) * UNIT).astype(BF16)

        def block(j, carry):
            part = jnp.dot(rotated, wts[j], preferred_element_type=F32)
            p[k, j] = part.reshape(4, 2, 8, COLS)
            p_copy(k, j).start()
            return carry

        lax.fori_loop(0, BLOCKS, block, 0)

    def reduce(k):
        def block(j, carry):
            p_copy(k, j).wait_recv()
            q[k, j] = (p[k, j, :, c] + pr[k, j]).astype(BF16)
            for d in range(3):
                q_copy(k, j, d).start()
            return carry

        lax.fori_loop(0, BLOCKS, block, 0)

    def gather(k):
        if k >= 2:
            await_bytes(r1r.at[k - 2], o_r.at[k - 2])

        def block(j, carry):
            total = p[k, j, y, c] + pr[k, j, y]
            await_bytes(qr.at[k, j], q_r.at[k, j])
            for d in range(3):
                total = total + qr[k, j, d].astype(F32)
            if k < 2:
                r1[k, j] = total.astype(BF16)
                o_copy(k, j).start()
            else:
                acc[k - 2, j] = total + r1r[k - 2, j].astype(F32)
            return carry

        lax.fori_loop(0, BLOCKS, block, 0)

    def finish(s):
        square = jnp.zeros((8, 1), F32)
        for j in range(BLOCKS):
            lanes = slice(j * COLS, (j + 1) * COLS)
            new = (res[s, :, lanes].astype(F32) + acc[s, j] * BRANCH).astype(BF16)
            new_out[s, :, lanes] = new
            values = new.astype(F32)
            square = square + jnp.sum(values * values, axis=1, keepdims=True)
        factor = lax.rsqrt(square * (1.0 / D) + 1e-05)
        for j in range(BLOCKS):
            lanes = slice(j * COLS, (j + 1) * COLS)
            norm_out[s, :, lanes] = (new_out[s, :, lanes].astype(F32) * factor).astype(BF16)

    spread(0)
    spread(1)
    spread(2)
    spread(3)

    @pl.when(z == 1)
    def _():
        lax.fori_loop(0, LOCAL // 16, dequantize, 0)

    turn(0)
    turn(1)
    turn(2)
    loads[4].wait()
    rotate(0)
    zin_copies[1].start()
    turn(3)
    rotate(1)
    rotate(2)
    rotate(3)
    receive(0)
    zin_copies[2].start()
    spread_far()
    spread(4)
    turn(4)
    zin_copies[3].start()
    multiply(0)
    reduce(0)
    receive(1)
    multiply(1)
    reduce(1)
    receive(2)
    gather(0)
    multiply(2)
    reduce(2)
    gather(1)
    receive(3)
    multiply(3)
    reduce(3)
    loads[5].wait()
    gather(2)
    finish(0)
    gather(3)
    finish(1)
    for landed, sent in ((zin, zin_s), (vr, v_s), (wr, w_s), (ub, u_s), (pr, p_s), (qr, q_s), (r1r, o_s)):
        await_bytes(landed, sent)


def local(hidden, signs, packed, group_scales, residual):
    table = jnp.asarray(np.kron(sylvester(LOCAL // 28), paley_table()), BF16)
    sem = pltpu.SemaphoreType.DMA
    outs = pl.pallas_call(
        kernel,
        out_shape=[jax.ShapeDtypeStruct((2, 8, D), BF16)] * 2,
        in_specs=[pl.BlockSpec(memory_space=pltpu.HBM)] * 6,
        out_specs=[pl.BlockSpec(memory_space=pltpu.VMEM)] * 2,
        scratch_shapes=[
            pltpu.VMEM((2, 4, 2, 2, 8, LOCAL), BF16),
            pltpu.VMEM((CHUNKS, 4, 2, 8, LOCAL), BF16),
            pltpu.VMEM((2, GROUPS, 128), jnp.int32),
            pltpu.VMEM((LOCAL, WORDS), jnp.int32),
            pltpu.VMEM((GROUPS, D), jnp.int32),
            pltpu.VMEM((2, 8, D), BF16),
            pltpu.VMEM((LOCAL, LOCAL), BF16),
            pltpu.VMEM((BLOCKS, LOCAL, COLS), BF16),
            pltpu.VMEM((5, 4, 2, 8, LOCAL), BF16),
            pltpu.VMEM((5, 4, 2, 8, LOCAL), BF16),
            pltpu.VMEM((5, 4, 2, 8, LOCAL), BF16),
            pltpu.VMEM((5, 3, 2, 8, LOCAL), BF16),
            pltpu.VMEM((5, 3, 2, 8, LOCAL), BF16),
            pltpu.VMEM((5, 4, 2, 8, LOCAL), BF16),
            pltpu.VMEM((4, 64, LOCAL), F32),
            pltpu.VMEM((3, 4, 2, 8, LOCAL), BF16),
            pltpu.VMEM((CHUNKS, BLOCKS, 4, 2, 8, COLS), F32),
            pltpu.VMEM((CHUNKS, BLOCKS, 4, 8, COLS), F32),
            pltpu.VMEM((CHUNKS, BLOCKS, 4, 8, COLS), BF16),
            pltpu.VMEM((CHUNKS, BLOCKS, 3, 8, COLS), BF16),
            pltpu.VMEM((2, BLOCKS, 8, COLS), BF16),
            pltpu.VMEM((2, BLOCKS, 8, COLS), BF16),
            pltpu.VMEM((2, BLOCKS, 8, COLS), F32),
            sem((6,)),
            sem,
            sem((CHUNKS,)),
            sem,
            sem,
            sem,
            sem((5,)),
            sem,
            sem((5,)),
            sem,
            sem((5,)),
            sem,
            sem((CHUNKS, BLOCKS)),
            sem,
            sem((CHUNKS, BLOCKS)),
            sem,
            sem((2,)),
        ],
        compiler_params=pltpu.CompilerParams(
            collective_id=0, has_side_effects=True, vmem_limit_bytes=56180000
        ),
        name="rotated_down",
    )(
        hidden.reshape(2, 4, 2, 2, 8, LOCAL),
        signs.reshape(GROUPS, 128),
        packed,
        group_scales,
        residual.reshape(2, 8, D),
        table,
    )
    return tuple(out.reshape(16, D) for out in outs)


def solution(mesh):
    in_specs = (P("dp", "tensor"), P("tensor"), P("tensor", None), P("tensor", None), P(("dp", "tensor"), None))
    out_specs = (P(("dp", "tensor"), None), P(("dp", "tensor"), None))
    return jax.shard_map(local, mesh=mesh, in_specs=in_specs, out_specs=out_specs, check_vma=False)
```
